32 devices in a mesh: dom: 16 (over z, y, x), mem: 2 (over core).
Axes of the slice: x: 2, y: 2, z: 4, core: 2. Of those that a mesh axis runs over, the one named last changes fastest.
Arguments:
- node_latents: bfloat16 [4, 2048, 512], P('mem', 'dom'), may hold values from -6 to 6
- edge_latents: bfloat16 [4, 8192, 512], P('mem', 'dom'), may hold values from -6 to 6
- edge_senders: int32 [8192], P('dom'), may hold values from 0 to 191, as said below
- edge_receivers: int32 [8192], P('dom'), may hold values from 0 to 127
- edge_counts: int32 [16], P('dom'), may hold values from 64 to 512, as said below
- halo_send: int32 [512], P('dom'), may hold values from 0 to 127
- long_send: int32 [16, 16, 2], replicated, may hold values from 0 to 3
- edge_first: bfloat16 [2, 1536, 512], P(None, None, 'mem'), may hold values from -0.15625 to 0.15625
- edge_second: bfloat16 [2, 512, 512], P(None, None, 'mem'), may hold values from -0.25 to 0.25
- node_first: bfloat16 [2, 1024, 512], P(None, None, 'mem'), may hold values from -0.1875 to 0.1875
- node_second: bfloat16 [2, 512, 512], P(None, None, 'mem'), may hold values from -0.25 to 0.25
- edge_gain: float32 [2, 512], replicated, may hold values from 0.5 to 1.5
- edge_shift: float32 [2, 512], replicated, may hold values from -3 to 3
- node_gain: float32 [2, 512], replicated, may hold values from 0.5 to 1.5
- node_shift: float32 [2, 512], replicated, may hold values from -3 to 3
Outputs:
- node_out: bfloat16 [4, 2048, 512], P('mem', 'dom')
- edge_out: bfloat16 [4, 8192, 512], P('mem', 'dom')
The draws below stay inside these ranges and needn't reach their ends.
Inputs may be any that keep to these rules, and one draw needn't show every extreme that they name: `edge_senders`: rows below 128 are the partition's own nodes, the next 32 its neighbours' sent nodes, the rest the coarse slots of all partitions. `edge_counts`: live slots come first in each partition; some partition has exactly 512 live slots.
All inputs are finite; a program needn't handle non-finite values.
Results may differ from the reference program's by a relative error of at most 0.0075.
Values may be sent and summed in bfloat16 or wider, within the bound.
A program may use at most 128 MiB of HBM per device.

```python
import jax
import jax.numpy as jnp
from jax import lax

D = 512
NODE_DEV = 128
EDGE_DEV = 512
HALO = 16
COARSE_DEV = 4
LONG_SLOT = 2
LAYERS = 2
MEMBERS = 4
NODES = 2048
EDGES = 8192
N_DOM = 16


def draw_edge_senders(key, part):
    kind_key = jax.random.fold_in(key, 11)
    local_key = jax.random.fold_in(key, 12)
    halo_key = jax.random.fold_in(key, 13)
    far_key = jax.random.fold_in(key, 14)
    total = N_DOM * EDGE_DEV
    kinds = jax.random.randint(kind_key, (total,), 0, 20)
    local_rows = jax.random.randint(local_key, (total,), 0, NODE_DEV)
    halo_rows = NODE_DEV + jax.random.randint(halo_key, (total,), 0, 2 * HALO)
    far_rows = NODE_DEV + 2 * HALO + jax.random.randint(far_key, (total,), 0, N_DOM * LONG_SLOT)
    picked = jnp.where(kinds < 14, local_rows, jnp.where(kinds < 17, halo_rows, far_rows))
    return picked.astype(jnp.int32)


def draw_edge_counts(key, part):
    count_key = jax.random.fold_in(key, 21)
    place_key = jax.random.fold_in(key, 22)
    counts = jax.random.randint(count_key, (N_DOM,), EDGE_DEV // 8, EDGE_DEV + 1)
    fullest = jax.random.randint(place_key, (), 0, N_DOM)
    counts = jnp.where(jnp.arange(N_DOM) == fullest, EDGE_DEV, counts)
    return counts.astype(jnp.int32)


def set_ends(values, stream_key, smallest, top_value):
    longest = values.shape.index(max(values.shape))
    spots = []
    for shift in (0, 1):
        where = [jax.random.randint(jax.random.fold_in(stream_key, axis), (), 0, length) for axis, length in enumerate(values.shape)]
        where[longest] = (where[longest] + shift) % values.shape[longest]
        spots.append(tuple(where))
    return values.at[spots[0]].set(smallest).at[spots[1]].set(top_value)


def block_levels(stream_key, dims, pieces, least, high):
    def one(dim, blocks):
        heights = jax.random.uniform(jax.random.fold_in(jax.random.fold_in(stream_key, 6), dim), (blocks,), jnp.float32, least / len(pieces), high / len(pieces))
        return jnp.repeat(jnp.exp(heights), dims[dim] // blocks).reshape((-1,) + (1,) * (len(dims) - dim - 1))

    gain = one(*pieces[0])
    for cut in pieces[1:]:
        gain = gain * one(*cut)
    return gain


def noise(stream_key, shape, deviation, most, shards=(), kind=jnp.bfloat16):
    factor_of = block_levels(stream_key, shape, shards, -0.22, 0.18) if shards else 1.0
    drawn = jax.random.normal(stream_key, shape, jnp.float32) * deviation * factor_of
    return jnp.minimum(jnp.maximum(drawn, -most), most).astype(kind)


def setup_inputs(seed: int = 0) -> dict:
    seeds = jax.random.split(jax.random.key(seed), 16)
    node_latents = noise(seeds[0], (MEMBERS, NODES, D), 1.0, 6.0, ((0, 2), (1, 16)))
    edge_latents = noise(seeds[1], (MEMBERS, EDGES, D), 1.0, 6.0, ((0, 2), (1, 16)))
    edge_senders = draw_edge_senders(jax.random.fold_in(seeds[15], 71), 0)
    edge_receivers = set_ends(jax.random.randint(seeds[3], (EDGES,), 0, NODE_DEV), jax.random.fold_in(seeds[3], 1), 0, NODE_DEV - 1).astype(jnp.int32)
    edge_counts = draw_edge_counts(jax.random.fold_in(seeds[15], 71), 0)
    halo_send = set_ends(jax.random.randint(seeds[5], (N_DOM * 2 * HALO,), 0, NODE_DEV), jax.random.fold_in(seeds[5], 1), 0, NODE_DEV - 1).astype(jnp.int32)
    long_send = set_ends(jax.random.randint(seeds[6], (N_DOM, N_DOM, LONG_SLOT), 0, COARSE_DEV), jax.random.fold_in(seeds[6], 1), 0, COARSE_DEV - 1).astype(jnp.int32)
    edge_first = noise(seeds[7], (LAYERS, 3 * D, D), (3 * D) ** -0.5, 0.15625, ((2, 2),))
    edge_second = noise(seeds[8], (LAYERS, D, D), D ** -0.5, 0.25, ((2, 2),))
    node_first = noise(seeds[9], (LAYERS, 2 * D, D), (2 * D) ** -0.5, 0.1875, ((2, 2),))
    node_second = noise(seeds[10], (LAYERS, D, D), D ** -0.5, 0.25, ((2, 2),))
    edge_gain = jnp.clip(1.0 + 0.1 * jax.random.normal(seeds[11], (LAYERS, D), jnp.float32), 0.5, 1.5)
    edge_shift = noise(seeds[12], (LAYERS, D), 0.5, 3.0, (), jnp.float32)
    node_gain = jnp.clip(1.0 + 0.1 * jax.random.normal(seeds[13], (LAYERS, D), jnp.float32), 0.5, 1.5)
    node_shift = noise(seeds[14], (LAYERS, D), 0.5, 3.0, (), jnp.float32)
    return {"node_latents": node_latents, "edge_latents": edge_latents, "edge_senders": edge_senders, "edge_receivers": edge_receivers, "edge_counts": edge_counts, "halo_send": halo_send, "long_send": long_send, "edge_first": edge_first, "edge_second": edge_second, "node_first": node_first, "node_second": node_second, "edge_gain": edge_gain, "edge_shift": edge_shift, "node_gain": node_gain, "node_shift": node_shift}


def project_norm(inputs, first_weight, second, scale_gain, offset):
    hidden = jax.nn.silu(jnp.dot(inputs, first_weight, preferred_element_type=jnp.float32)).astype(jnp.bfloat16)
    output = jnp.dot(hidden, second, preferred_element_type=jnp.float32)
    average = lax.optimization_barrier(jnp.mean(output, -1, keepdims=True))
    centred = output - average
    variance = lax.optimization_barrier(jnp.mean(centred * centred, -1, keepdims=True))
    return centred * lax.rsqrt(variance + 1e-05) * scale_gain + offset

def reference(node_latents, edge_latents, edge_senders, edge_receivers, edge_counts, halo_send, long_send, edge_first, edge_second, node_first, node_second, edge_gain, edge_shift, node_gain, node_shift):
    partitions = N_DOM
    node_rows = NODE_DEV
    edge_rows = EDGE_DEV
    features = D
    members = node_latents.shape[0]
    halo_rows = halo_send.reshape(partitions, 2 * HALO)
    partition_ids = jnp.arange(partitions, dtype=jnp.int32)
    own_ids = partition_ids[:, None] * node_rows + jnp.arange(node_rows, dtype=jnp.int32)[None, :]
    previous = (partition_ids - 1) % partitions
    following = (partition_ids + 1) % partitions
    left_ids = previous[:, None] * node_rows + halo_rows[previous][:, HALO:]
    right_ids = following[:, None] * node_rows + halo_rows[following][:, :HALO]
    far_ids = partition_ids[None, :, None] * node_rows + jnp.transpose(long_send, (1, 0, 2))
    far_ids = far_ids.reshape(partitions, partitions * LONG_SLOT)
    source_ids = jnp.concatenate([own_ids, left_ids, right_ids, far_ids], 1).astype(jnp.int32)
    senders = edge_senders.reshape(partitions, edge_rows)
    sender_ids = jnp.take_along_axis(source_ids, senders, axis=1)
    receivers = edge_receivers.reshape(partitions, edge_rows)
    node_state = node_latents
    edge_state = jnp.transpose(edge_latents.reshape(members, partitions, edge_rows, features), (1, 0, 2, 3))
    for layer_index in range(LAYERS):

        def one_part(part_item):
            snd_ids, rcv_ids, live_count, edge_block, node_block = part_item
            sender_rows = jnp.take(node_state, snd_ids, axis=1)
            receiver_rows = jnp.take(node_block, rcv_ids, axis=1)
            joined = jnp.concatenate([edge_block, sender_rows, receiver_rows], -1).reshape(members * edge_rows, 3 * features)
            update = project_norm(joined, edge_first[layer_index], edge_second[layer_index], edge_gain[layer_index], edge_shift[layer_index]).reshape(members, edge_rows, features)
            live_mask = jnp.arange(edge_rows, dtype=jnp.int32) < live_count
            new_edges = jnp.where(live_mask[None, :, None], edge_block.astype(jnp.float32) + update, 0.0).astype(jnp.bfloat16)
            onehot = ((rcv_ids[None, :] == jnp.arange(node_rows, dtype=jnp.int32)[:, None]) & live_mask[None, :]).astype(jnp.float32)
            summed = jnp.einsum('ne,med->mnd', onehot, new_edges.astype(jnp.float32)).astype(jnp.bfloat16)
            node_in = jnp.concatenate([node_block, summed], -1).reshape(members * node_rows, 2 * features)
            node_update = project_norm(node_in, node_first[layer_index], node_second[layer_index], node_gain[layer_index], node_shift[layer_index]).reshape(members, node_rows, features)
            new_nodes = (node_block.astype(jnp.float32) + node_update).astype(jnp.bfloat16)
            return (new_nodes, new_edges)
        node_blocks = jnp.transpose(node_state.reshape(members, partitions, node_rows, features), (1, 0, 2, 3))
        new_nodes, new_edges = lax.map(one_part, (sender_ids, receivers, edge_counts, edge_state, node_blocks))
        node_state = jnp.transpose(new_nodes, (1, 0, 2, 3)).reshape(members, partitions * node_rows, features)
        edge_state = new_edges
    edge_final = jnp.transpose(edge_state, (1, 0, 2, 3)).reshape(members, partitions * edge_rows, features)
    return (node_state, edge_final)
```

```python
import functools

import jax
import jax.numpy as jnp
from jax import lax
from jax.experimental import pallas as pl
from jax.experimental.pallas import tpu as pltpu
from jax.sharding import PartitionSpec as P

F32, BF16 = jnp.float32, jnp.bfloat16
LANES = 128
CHUNK = 256


def round_up(value, step):
    return (value + step - 1) // step * step


def dot(a, b):
    return jnp.dot(a, b, preferred_element_type=F32)


def silu(x):
    half = 0.5 * x
    return (half + half * jnp.tanh(half)).astype(BF16)


def norm(x, gain, shift):
    average = jnp.mean(x, -1, keepdims=True)
    centred = x - average
    variance = jnp.mean(centred * centred, -1, keepdims=True)
    return centred * lax.rsqrt(variance + 1e-05) * gain + shift


def kernel(
    sizes,
    node_in, edge_in, index_in, ef_in, es_in, nf_in, ns_in, eg_in, eb_in, ng_in, nb_in,
    node_out, edge_out,
    node, edge, index, w1, w2, w3, w4, eg, eb, ng, nb,
    gather, scatter, picker, table, near, pre, node_pre, summed,
    halo_out, halo, far_out, far, far_rows,
    local_sem, wl_sem, ws_sem, wr_sem, hs_sem, hr_sem, fs_sem, fr_sem,
):
    n, layers, members, nodes, edges, width, side_rows, slots, far_base = sizes
    me = lax.axis_index("dom")
    core = lax.axis_index("mem")
    halves = 2
    half = width // halves
    other = 1 - core

    barrier = pltpu.get_barrier_semaphore()
    pl.semaphore_signal(barrier, inc=1, device_id={"mem": other})
    for step in range(1, n):
        pl.semaphore_signal(barrier, inc=1, device_id={"dom": lax.rem(me + step, n)})

    loads = []
    for place, (src, dst) in enumerate(
        ((node_in, node), (index_in, index), (edge_in, edge), (eg_in, eg), (eb_in, eb), (ng_in, ng), (nb_in, nb))
    ):
        copy = pltpu.make_async_copy(src, dst, local_sem.at[place])
        copy.start()
        loads.append(copy)
    weights = ((ef_in, w1), (es_in, w2), (nf_in, w3), (ns_in, w4))
    own = {}
    for l in range(layers):
        for k, (src, dst) in enumerate(weights):
            own[l, k] = pltpu.make_async_copy(src.at[l], dst.at[l, core], wl_sem.at[l, k])
            own[l, k].start()

    loads[1].wait()
    depth = gather.shape[1]
    turned = jnp.transpose(jnp.broadcast_to(index[0:1, :], (LANES, index.shape[1])))
    senders = turned[:edges]
    receivers = turned[edges : 2 * edges] + nodes
    senders = jnp.where(senders < nodes, senders, senders + nodes)
    for c in range(depth // LANES):
        lane = lax.broadcasted_iota(jnp.int32, (edges, LANES), 1) + c * LANES
        gather[:, c * LANES : (c + 1) * LANES] = (
            ((senders == lane) | (receivers == lane)).astype(F32).astype(BF16)
        )
    row = lax.broadcasted_iota(jnp.int32, (nodes, edges), 0)
    scatter[...] = (
        (jnp.broadcast_to(index[0:1, edges : 2 * edges], (nodes, edges)) == row).astype(F32).astype(BF16)
    )
    pick_rows = picker.shape[0]
    base = 2 * edges + LANES
    for c in range(nodes // LANES):
        lane = lax.broadcasted_iota(jnp.int32, (pick_rows, LANES), 1) + c * LANES
        picker[:, c * LANES : (c + 1) * LANES] = (
            (turned[base : base + pick_rows] == lane).astype(F32).astype(BF16)
        )
    count = index[0:1, 2 * edges : 2 * edges + 1]
    for m in range(members):
        table[m, far_base:, :] = jnp.zeros((table.shape[1] - far_base, width), BF16)

    loads[0].wait()
    pending = []
    partner = {}
    for l in range(layers):
        for m in range(members):
            packed = dot(picker[...], node[m])
            for side in range(2):
                halo_out[l, side, m * side_rows : (m + 1) * side_rows, :] = packed[
                    side * side_rows : (side + 1) * side_rows
                ].astype(BF16)
            for q in range(n):
                start = 2 * side_rows + q * slots
                far_out[l, q, m * slots : (m + 1) * slots, :] = packed[start : start + slots].astype(BF16)
        if l == 0:
            pl.semaphore_wait(barrier, n)
        arrivals = []
        for side, step in ((1, 1), (0, n - 1)):
            copy = pltpu.make_async_remote_copy(
                src_ref=halo_out.at[l, side],
                dst_ref=halo.at[l, 1 - side],
                send_sem=hs_sem.at[l, side],
                recv_sem=hr_sem.at[l, side],
                device_id={"dom": lax.rem(me + step, n)},
            )
            copy.start()
            arrivals.append(copy)
        for step in range(1, n):
            target = lax.rem(me + step, n)
            copy = pltpu.make_async_remote_copy(
                src_ref=far_out.at[l, target],
                dst_ref=far.at[l, me],
                send_sem=fs_sem.at[l, step],
                recv_sem=fr_sem.at[l, step],
                device_id={"dom": target},
            )
            copy.start()
            arrivals.append(copy)
        mine = pltpu.make_async_copy(far_out.at[l, me], far.at[l, me], fr_sem.at[l, 0])
        mine.start()
        if l == 0:
            for ll in range(layers):
                for k, (src, dst) in enumerate(weights):
                    copy = pltpu.make_async_remote_copy(
                        src_ref=src.at[ll],
                        dst_ref=dst.at[ll, core],
                        send_sem=ws_sem.at[ll, k],
                        recv_sem=wr_sem.at[ll, k],
                        device_id={"mem": other},
                    )
                    copy.start()
                    partner[ll, k] = copy
                    pending.append(copy)
            loads[2].wait()
            for copy in loads[3:]:
                copy.wait()

        own[l, 0].wait()
        partner[l, 0].wait_recv()
        for h in range(halves):
            cols = slice(h * half, (h + 1) * half)
            stacked = node[...].reshape(members * nodes, width)
            by_sender = dot(stacked, w1[l, h, width : 2 * width, :]).astype(BF16)
            by_receiver = dot(stacked, w1[l, h, 2 * width :, :]).astype(BF16)
            for m in range(members):
                table[m, :nodes, cols] = by_sender[m * nodes : (m + 1) * nodes]
                table[m, nodes : 2 * nodes, cols] = by_receiver[m * nodes : (m + 1) * nodes]
        for m in range(members):
            for c in range(edges // CHUNK):
                rows = slice(c * CHUNK, (c + 1) * CHUNK)
                for h in range(halves):
                    cols = slice(h * half, (h + 1) * half)
                    pre[m, rows, cols] = dot(edge[m, rows, :], w1[l, h, :width, :]) + dot(
                        gather[rows, : 2 * nodes], table[m, : 2 * nodes, cols]
                    )
        own[l, 2].wait()
        partner[l, 2].wait_recv()
        for h in range(halves):
            cols = slice(h * half, (h + 1) * half)
            node_pre[:, cols] = dot(node[...].reshape(members * nodes, width), w3[l, h, :width, :])
        own[l, 1].wait()
        partner[l, 1].wait_recv()
        own[l, 3].wait()
        partner[l, 3].wait_recv()

        for copy in arrivals:
            copy.wait_recv()
        mine.wait()
        pending.extend(arrivals)
        for m in range(members):
            for side in range(2):
                near[m, side * side_rows : (side + 1) * side_rows, :] = halo[
                    l, side, m * side_rows : (m + 1) * side_rows, :
                ]
        for q in range(n):
            block = far[l, q].astype(F32)
            for m in range(members):
                far_rows[m, q * slots : (q + 1) * slots, :] = block[m * slots : (m + 1) * slots]
        for m in range(members):
            near[m, 2 * side_rows :, :] = far_rows[m].astype(BF16)
        count_near = near.shape[1]
        for h in range(halves):
            cols = slice(h * half, (h + 1) * half)
            moved = dot(near[...].reshape(members * count_near, width), w1[l, h, width : 2 * width, :]).astype(BF16)
            for m in range(members):
                table[m, 2 * nodes : 2 * nodes + count_near, cols] = moved[m * count_near : (m + 1) * count_near]

        for m in range(members):
            for c in range(edges // CHUNK):
                rows = slice(c * CHUNK, (c + 1) * CHUNK)
                hidden = silu(pre[m, rows, :] + dot(gather[rows, 2 * nodes :], table[m, 2 * nodes :, :]))
                out = jnp.concatenate([dot(hidden, w2[l, h]) for h in range(halves)], -1)
                update = norm(out, eg[l : l + 1, :], eb[l : l + 1, :])
                live = lax.broadcasted_iota(jnp.int32, (CHUNK, 1), 0) + c * CHUNK < count
                edge[m, rows, :] = jnp.where(live, edge[m, rows, :].astype(F32) + update, 0.0).astype(BF16)
            summed[m * nodes : (m + 1) * nodes, :] = dot(scatter[...], edge[m]).astype(BF16)
        if l == layers - 1:
            edge_store = pltpu.make_async_copy(edge, edge_out, local_sem.at[2])
            edge_store.start()

        first = jnp.concatenate(
            [
                node_pre[:, h * half : (h + 1) * half] + dot(summed[...], w3[l, h, width:, :])
                for h in range(halves)
            ],
            -1,
        )
        hidden = silu(first)
        out = jnp.concatenate([dot(hidden, w4[l, h]) for h in range(halves)], -1)
        update = norm(out, ng[l : l + 1, :], nb[l : l + 1, :])
        for m in range(members):
            node[m] = (node[m].astype(F32) + update[m * nodes : (m + 1) * nodes]).astype(BF16)
    node_store = pltpu.make_async_copy(node, node_out, local_sem.at[0])
    node_store.start()
    for copy in pending:
        copy.wait_send()
    edge_store.wait()
    node_store.wait()


def solution(mesh):
    n = mesh.shape["dom"]

    def step(
        node, edge, senders, receivers, counts, halo_send, long_send, ef, es, nf, ns, eg, eb, ng, nb
    ):
        members, nodes, width = node.shape
        edges = edge.shape[1]
        layers = ef.shape[0]
        side_rows = halo_send.shape[0] // 2
        slots = long_send.shape[-1]
        me = lax.axis_index("dom")
        sent = lax.dynamic_index_in_dim(long_send, me, 0, keepdims=False).reshape(-1)
        near_rows = 2 * side_rows + n * slots
        pick_rows = near_rows
        fill = round_up(pick_rows, LANES) - pick_rows
        index = jnp.concatenate(
            [senders, receivers, jnp.broadcast_to(counts, (LANES,)), halo_send, sent, jnp.zeros((fill,), jnp.int32)]
        ).reshape(1, -1)
        depth = 2 * nodes + round_up(near_rows, LANES)
        sizes = (n, layers, members, nodes, edges, width, side_rows, slots, 2 * nodes + near_rows)
        half = width // 2
        hbm = pl.BlockSpec(memory_space=pl.ANY)
        dma = pltpu.SemaphoreType.DMA
        return pl.pallas_call(
            functools.partial(kernel, sizes),
            out_shape=(
                jax.ShapeDtypeStruct(node.shape, BF16),
                jax.ShapeDtypeStruct(edge.shape, BF16),
            ),
            in_specs=[hbm] * 11,
            out_specs=(hbm, hbm),
            scratch_shapes=[
                pltpu.VMEM(node.shape, BF16),
                pltpu.VMEM(edge.shape, BF16),
                pltpu.VMEM(index.shape, jnp.int32),
                pltpu.VMEM((layers, 2, ef.shape[1], half), BF16),
                pltpu.VMEM((layers, 2, es.shape[1], half), BF16),
                pltpu.VMEM((layers, 2, nf.shape[1], half), BF16),
                pltpu.VMEM((layers, 2, ns.shape[1], half), BF16),
                pltpu.VMEM(eg.shape, F32),
                pltpu.VMEM(eb.shape, F32),
                pltpu.VMEM(ng.shape, F32),
                pltpu.VMEM(nb.shape, F32),
                pltpu.VMEM((edges, depth), BF16),
                pltpu.VMEM((nodes, edges), BF16),
                pltpu.VMEM((pick_rows, nodes), BF16),
                pltpu.VMEM((members, depth, width), BF16),
                pltpu.VMEM((members, near_rows, width), BF16),
                pltpu.VMEM((members, edges, width), F32),
                pltpu.VMEM((members * nodes, width), F32),
                pltpu.VMEM((members * nodes, width), BF16),
                pltpu.VMEM((layers, 2, members * side_rows, width), BF16),
                pltpu.VMEM((layers, 2, members * side_rows, width), BF16),
                pltpu.VMEM((layers, n, members * slots, width), BF16),
                pltpu.VMEM((layers, n, members * slots, width), BF16),
                pltpu.VMEM((members, n * slots, width), F32),
                dma((7,)),
                dma((layers, 4)),
                dma((layers, 4)),
                dma((layers, 4)),
                dma((layers, 2)),
                dma((layers, 2)),
                dma((layers, n)),
                dma((layers, n)),
            ],
            compiler_params=pltpu.CompilerParams(
                collective_id=0, has_side_effects=True, vmem_limit_bytes=56 * 1024 * 1024
            ),
        )(node, edge, index, ef, es, nf, ns, eg, eb, ng, nb)

    placed = (
        P("mem", "dom", None),
        P("mem", "dom", None),
        P("dom"),
        P("dom"),
        P("dom"),
        P("dom"),
        P(),
        P(None, None, "mem"),
        P(None, None, "mem"),
        P(None, None, "mem"),
        P(None, None, "mem"),
        P(),
        P(),
        P(),
        P(),
    )
    return jax.shard_map(
        step,
        mesh=mesh,
        in_specs=placed,
        out_specs=(P("mem", "dom", None), P("mem", "dom", None)),
        check_vma=False,
    )
```

```python
import functools

import jax
import jax.numpy as jnp
from jax import lax
from jax.experimental import pallas as pl
from jax.experimental.pallas import tpu as pltpu
from jax.sharding import PartitionSpec as P

F32, BF16 = jnp.float32, jnp.bfloat16
LANES = 128
CHUNK = 256


def round_up(value, step):
    return (value + step - 1) // step * step


def dot(a, b):
    return jnp.dot(a, b, preferred_element_type=F32)


def silu(x):
    half = 0.5 * x
    return (half + half * jnp.tanh(half)).astype(BF16)


def norm(x, gain, shift):
    average = jnp.mean(x, -1, keepdims=True)
    centred = x - average
    variance = jnp.mean(centred * centred, -1, keepdims=True)
    return centred * lax.rsqrt(variance + 1e-05) * gain + shift


def edge_update(m, edges, refs):
    edge, pre, table, gather, scatter, w2, eg, eb, count, split = refs
    halves = pre.shape[0]
    for c in range(edges // CHUNK):
        rows = slice(c * CHUNK, (c + 1) * CHUNK)
        hidden = jnp.concatenate(
            [silu(pre[h, m, rows, :] + dot(gather[rows, split:], table[h, m, split:, :])) for h in range(halves)], -1
        )
        out = jnp.concatenate([dot(hidden, w2[h]) for h in range(halves)], -1)
        update = norm(out, eg, eb)
        live = lax.broadcasted_iota(jnp.int32, (CHUNK, 1), 0) + c * CHUNK < count
        edge[m, rows, :] = jnp.where(live, edge[m, rows, :].astype(F32) + update, 0.0).astype(BF16)
    return dot(scatter[...], edge[m]).astype(BF16)


def node_update(m, summed, refs):
    node, node_pre, w3, w4, ng, nb = refs
    halves, half = w4.shape[0], w4.shape[2]
    width = half * halves
    hidden = jnp.concatenate(
        [silu(node_pre[h, m] + dot(summed, w3[h, width:, :])) for h in range(halves)], -1
    )
    out = jnp.concatenate([dot(hidden, w4[h]) for h in range(halves)], -1)
    node[m] = (node[m].astype(F32) + norm(out, ng, nb)).astype(BF16)


def exchange_kernel(
    sizes,
    node_in, edge_in, senders_in, receivers_in, counts_in, halo_in, long_in,
    ef_in, es_in, nf_in, ns_in, eg_in, eb_in, ng_in, nb_in,
    node, edge, pre, node_pre, table, gather, scatter, w2, w3, w4, eg, eb, ng, nb, count_row,
    w1, senders_v, receivers_v, count_s, halo_v, long_v, picked, picker, near, far_rows,
    halo_out, halo, far_out, far,
    local_sem, wl_sem, ws_sem, wr_sem, hs_sem, hr_sem, fs_sem, fr_sem,
):
    n, layers, members, nodes, edges, width, side_rows, slots = sizes
    me = lax.axis_index("dom")
    core = lax.axis_index("mem")
    halves = 2
    other = 1 - core
    split = 2 * nodes

    barrier = pltpu.get_barrier_semaphore()
    pl.semaphore_signal(barrier, inc=1, device_id={"mem": other})
    for step in range(1, n):
        pl.semaphore_signal(barrier, inc=1, device_id={"dom": lax.rem(me + step, n)})

    loads = []
    for place, (src, dst) in enumerate((
        (node_in, node), (halo_in, halo_v), (long_in.at[me], long_v), (senders_in, senders_v),
        (receivers_in, receivers_v), (counts_in, count_s), (edge_in, edge),
        (eg_in, eg), (eb_in, eb), (ng_in, ng), (nb_in, nb),
    )):
        copy = pltpu.make_async_copy(src, dst, local_sem.at[place])
        loads.append(copy)
    weights = ((ef_in, w1), (es_in, w2), (nf_in, w3), (ns_in, w4))
    own = {}
    for l in range(layers):
        for k, (src, dst) in enumerate(weights):
            own[l, k] = pltpu.make_async_copy(src.at[l], dst.at[l, core], wl_sem.at[l, k])
    for copy in loads[:6]:
        copy.start()
    own[0, 0].start()
    loads[6].start()
    for place in loads[7:]:
        place.start()
    for key in own:
        if key != (0, 0):
            own[key].start()

    def column(row):
        wide = round_up(row.shape[1], LANES)
        if wide > row.shape[1]:
            row = jnp.concatenate([row, jnp.zeros((1, wide - row.shape[1]), jnp.int32)], 1)
        return jnp.transpose(jnp.broadcast_to(row, (LANES, wide)))

    def one_hot(hits):
        return hits.astype(F32).astype(BF16)

    loads[1].wait()
    loads[2].wait()
    picked[: 2 * side_rows, :] = column(halo_v[...].reshape(1, 2 * side_rows))[: 2 * side_rows]
    for s in range(slots):
        picked[pl.ds(2 * side_rows + s, n, stride=slots), :] = column(long_v[s : s + 1, :])[:n]
    for c in range(nodes // LANES):
        lane = lax.broadcasted_iota(jnp.int32, picked.shape, 1) + c * LANES
        picker[:, c * LANES : (c + 1) * LANES] = one_hot(picked[...] == lane)

    pending = []
    arrivals = {}

    def send(l, m):
        packed = dot(picker[...], node[m])
        for side in range(2):
            halo_out[l, m, side] = packed[side * side_rows : (side + 1) * side_rows].astype(BF16)
        for q in range(n):
            start = 2 * side_rows + q * slots
            far_out[l, m, q] = packed[start : start + slots].astype(BF16)
        if l == 0 and m == 0:
            pl.semaphore_wait(barrier, n)
        copies = []
        for step in range(1, n):
            target = lax.rem(me + step, n)
            copies.append(pltpu.make_async_remote_copy(
                src_ref=far_out.at[l, m, target],
                dst_ref=far.at[l, m, me],
                send_sem=fs_sem.at[l, m, step],
                recv_sem=fr_sem.at[l, m, step],
                device_id={"dom": target},
            ))
        for side, step in ((1, 1), (0, n - 1)):
            copies.append(pltpu.make_async_remote_copy(
                src_ref=halo_out.at[l, m, side],
                dst_ref=halo.at[l, m, 1 - side],
                send_sem=hs_sem.at[l, m, side],
                recv_sem=hr_sem.at[l, m, side],
                device_id={"dom": lax.rem(me + step, n)},
            ))
        for copy in copies:
            copy.start()
        mine = pltpu.make_async_copy(far_out.at[l, m, me], far.at[l, m, me], fr_sem.at[l, m, 0])
        mine.start()
        pending.extend(copies)
        arrivals[l, m] = (copies, mine)

    def prepare(l, h, ms):
        for m in ms:
            table[h, m, :nodes, :] = dot(node[m], w1[l, h, width : 2 * width, :]).astype(BF16)
            table[h, m, nodes:split, :] = dot(node[m], w1[l, h, 2 * width :, :]).astype(BF16)
        for m in ms:
            pre[h, m] = dot(edge[m], w1[l, h, :width, :]) + dot(gather[:, :split], table[h, m, :split, :])

    def node_prepare(l, m):
        for h in range(halves):
            node_pre[h, m] = dot(node[m], w3[l, h, :width, :])

    def receive(l, m):
        copies, mine = arrivals[l, m]
        for copy in copies:
            copy.wait_recv()
        mine.wait()
        for side in range(2):
            near[m, side * side_rows : (side + 1) * side_rows, :] = halo[l, m, side]
        for q in range(n):
            far_rows[m, q * slots : (q + 1) * slots, :] = far[l, m, q].astype(F32)
        near[m, 2 * side_rows :, :] = far_rows[m].astype(BF16)
        count_near = near.shape[1]
        for h in range(halves):
            table[h, m, split : split + count_near, :] = dot(near[m], w1[l, h, width : 2 * width, :]).astype(BF16)

    loads[0].wait()
    for m in range(members):
        send(0, m)
    partner = {}
    for l in range(layers):
        for k, (src, dst) in enumerate(weights):
            copy = pltpu.make_async_remote_copy(
                src_ref=src.at[l],
                dst_ref=dst.at[l, core],
                send_sem=ws_sem.at[l, k],
                recv_sem=wr_sem.at[l, k],
                device_id={"mem": other},
            )
            copy.start()
            partner[l, k] = copy
            pending.append(copy)

    loads[3].wait()
    loads[4].wait()
    depth = gather.shape[1]
    senders = column(senders_v[...].reshape(1, edges))
    receiver_row = receivers_v[...].reshape(1, edges)
    receivers = column(receiver_row) + nodes
    senders = jnp.where(senders < nodes, senders, senders + nodes)
    for c in range(depth // LANES):
        lane = lax.broadcasted_iota(jnp.int32, (edges, LANES), 1) + c * LANES
        gather[:, c * LANES : (c + 1) * LANES] = one_hot((senders == lane) | (receivers == lane))
    row = lax.broadcasted_iota(jnp.int32, (nodes, edges), 0)
    scatter[...] = one_hot(jnp.broadcast_to(receiver_row, (nodes, edges)) == row)
    far_base = split + near.shape[1]
    if far_base < depth:
        for h in range(halves):
            for m in range(members):
                table[h, m, far_base:, :] = jnp.zeros((depth - far_base, table.shape[3]), BF16)
    loads[5].wait()
    count_row[...] = jnp.full(count_row.shape, count_s[0], jnp.int32)
    for copy in loads[6:]:
        copy.wait()
    own[0, 0].wait()
    everyone = range(members)
    prepare(0, core, everyone)
    partner[0, 0].wait_recv()
    prepare(0, other, everyone)
    for k in (1, 2, 3):
        own[0, k].wait()
        partner[0, k].wait_recv()
    for m in everyone:
        node_prepare(0, m)

    for l in range(layers):
        if l > 0:
            own[l, 0].wait()
            partner[l, 0].wait_recv()
            for h in range(halves):
                prepare(l, h, everyone)
            for k in (1, 2, 3):
                own[l, k].wait()
                partner[l, k].wait_recv()
            for m in everyone:
                node_prepare(l, m)
        for m in everyone:
            receive(l, m)
            if l == layers - 1 and m == members - 1:
                continue
            summed = edge_update(m, edges, (
                edge, pre, table, gather, scatter, w2.at[l], eg[l : l + 1, :], eb[l : l + 1, :],
                count_row[0:1, 0:1], split,
            ))
            node_update(m, summed, (node, node_pre, w3.at[l], w4.at[l], ng[l : l + 1, :], nb[l : l + 1, :]))
            if l < layers - 1:
                send(l + 1, m)
    for copy in pending:
        copy.wait_send()


def finish_kernel(
    sizes,
    node, edge, pre, node_pre, table, gather, scatter, w2, w3, w4, eg, eb, ng, nb, count_row,
    node_out, edge_out, edge_new, node_new, sem,
):
    n, layers, members, nodes, edges, width, side_rows, slots = sizes
    l, m = layers - 1, members - 1
    copies = []

    def store(src, dst):
        copy = pltpu.make_async_copy(src, dst, sem.at[len(copies)])
        copy.start()
        copies.append(copy)

    store(edge.at[:m], edge_out.at[:m])
    store(node.at[:m], node_out.at[:m])
    halves = pre.shape[0]
    split = 2 * nodes
    total = None
    count = count_row[0:1, 0:1]
    for c in range(edges // CHUNK):
        rows = slice(c * CHUNK, (c + 1) * CHUNK)
        hidden = jnp.concatenate(
            [silu(pre[h, m, rows, :] + dot(gather[rows, split:], table[h, m, split:, :])) for h in range(halves)], -1
        )
        out = jnp.concatenate([dot(hidden, w2[l, h]) for h in range(halves)], -1)
        update = norm(out, eg[l : l + 1, :], eb[l : l + 1, :])
        live = lax.broadcasted_iota(jnp.int32, (CHUNK, 1), 0) + c * CHUNK < count
        edge_new[rows, :] = jnp.where(live, edge[m, rows, :].astype(F32) + update, 0.0).astype(BF16)
        store(edge_new.at[rows], edge_out.at[m, rows])
    summed = dot(scatter[...], edge_new[...]).astype(BF16)
    hidden = jnp.concatenate(
        [silu(node_pre[h, m] + dot(summed, w3[l, h, width:, :])) for h in range(halves)], -1
    )
    out = jnp.concatenate([dot(hidden, w4[l, h]) for h in range(halves)], -1)
    update = norm(out, ng[l : l + 1, :], nb[l : l + 1, :])
    node_new[...] = (node[m].astype(F32) + update).astype(BF16)
    store(node_new, node_out.at[m])
    for copy in copies:
        copy.wait()


def solution(mesh):
    n = mesh.shape["dom"]

    def step(
        node, edge, senders, receivers, counts, halo_send, long_send, ef, es, nf, ns, eg, eb, ng, nb
    ):
        members, nodes, width = node.shape
        edges = edge.shape[1]
        layers = ef.shape[0]
        side_rows = halo_send.shape[0] // 2
        slots = long_send.shape[-1]
        long_rows = jnp.swapaxes(long_send, 1, 2)
        near_rows = 2 * side_rows + n * slots
        depth = 2 * nodes + round_up(near_rows, LANES)
        sizes = (n, layers, members, nodes, edges, width, side_rows, slots)
        half = width // 2
        hbm = pl.BlockSpec(memory_space=pltpu.HBM)
        vmem = pl.BlockSpec(memory_space=pltpu.VMEM)
        dma = pltpu.SemaphoreType.DMA
        kept = [
            (node.shape, BF16),
            (edge.shape, BF16),
            ((2, members, edges, half), F32),
            ((2, members, nodes, half), F32),
            ((2, members, depth, half), BF16),
            ((edges, depth), BF16),
            ((nodes, edges), BF16),
            ((layers, 2, es.shape[1], half), BF16),
            ((layers, 2, nf.shape[1], half), BF16),
            ((layers, 2, ns.shape[1], half), BF16),
            (eg.shape, F32),
            (eb.shape, F32),
            (ng.shape, F32),
            (nb.shape, F32),
            ((1, LANES), jnp.int32),
        ]
        state = pl.pallas_call(
            functools.partial(exchange_kernel, sizes),
            out_shape=tuple(pltpu.VMEM(shape, kind) for shape, kind in kept),
            in_specs=[hbm] * 15,
            out_specs=(vmem,) * len(kept),
            scratch_shapes=[
                pltpu.VMEM((layers, 2, ef.shape[1], half), BF16),
                pltpu.VMEM(senders.shape, jnp.int32),
                pltpu.VMEM(receivers.shape, jnp.int32),
                pltpu.SMEM(counts.shape, jnp.int32),
                pltpu.VMEM(halo_send.shape, jnp.int32),
                pltpu.VMEM(long_rows.shape[1:], jnp.int32),
                pltpu.VMEM((near_rows, LANES), jnp.int32),
                pltpu.VMEM((near_rows, nodes), BF16),
                pltpu.VMEM((members, near_rows, width), BF16),
                pltpu.VMEM((members, n * slots, width), F32),
                pltpu.VMEM((layers, members, 2, side_rows, width), BF16),
                pltpu.VMEM((layers, members, 2, side_rows, width), BF16),
                pltpu.VMEM((layers, members, n, slots, width), BF16),
                pltpu.VMEM((layers, members, n, slots, width), BF16),
                dma((11,)),
                dma((layers, 4)),
                dma((layers, 4)),
                dma((layers, 4)),
                dma((layers, members, 2)),
                dma((layers, members, 2)),
                dma((layers, members, n)),
                dma((layers, members, n)),
            ],
            compiler_params=pltpu.CompilerParams(
                collective_id=0, has_side_effects=True, vmem_limit_bytes=51 * 1024 * 1024
            ),
        )(node, edge, senders, receivers, counts, halo_send, long_rows, ef, es, nf, ns, eg, eb, ng, nb)
        return pl.pallas_call(
            functools.partial(finish_kernel, sizes),
            out_shape=(
                jax.ShapeDtypeStruct(node.shape, BF16),
                jax.ShapeDtypeStruct(edge.shape, BF16),
            ),
            in_specs=[vmem] * len(kept),
            out_specs=(hbm, hbm),
            scratch_shapes=[
                pltpu.VMEM((edges, width), BF16),
                pltpu.VMEM((nodes, width), BF16),
                dma((3 + edges // CHUNK,)),
            ],
            compiler_params=pltpu.CompilerParams(vmem_limit_bytes=40 * 1024 * 1024),
        )(*state)

    placed = (
        P("mem", "dom", None),
        P("mem", "dom", None),
        P("dom"),
        P("dom"),
        P("dom"),
        P("dom"),
        P(),
        P(None, None, "mem"),
        P(None, None, "mem"),
        P(None, None, "mem"),
        P(None, None, "mem"),
        P(),
        P(),
        P(),
        P(),
    )
    return jax.shard_map(
        step,
        mesh=mesh,
        in_specs=placed,
        out_specs=(P("mem", "dom", None), P("mem", "dom", None)),
        check_vma=False,
    )
```
